32 devices in a mesh: sta: 16 (over z, x, core), tm: 2 (over y).
Axes of the slice: x: 2, y: 2, z: 4, core: 2. Of those that a mesh axis runs over, the one named last changes fastest.
Arguments:
- records: bfloat16 [32, 3, 1024], P('sta', None, 'tm'), may hold values from -6 to 6
- templates: bfloat16 [512, 32, 3, 150], P(None, 'sta'), may hold values from -6 to 6
- moveout: int32 [512, 32], P(None, 'sta'), may hold values from 0 to 256
- gap_start: int32 [32, 3], P('sta'), may hold values from 0 to 1023
- gap_length: int32 [32, 3], P('sta'), may hold values from 0 to 599
Outputs:
- detection: float32 [512, 1024], P('sta', 'tm')
The draws below stay inside these ranges and needn't reach their ends.
Inputs may be any that keep to these rules, and one draw needn't show every extreme that they name: `gap_length`: each channel has one gap, counted in samples of the whole window; it may run past the window's end.
All inputs are finite; a program needn't handle non-finite values.
Results may differ from the reference program's by a relative error of at most 0.0041.
Values may be sent and summed in bfloat16 or wider, within the bound.
No kernel may reach another device: no remote copies, remote signals or barrier semaphores. Data moves between devices by JAX's collectives and lax.ppermute only.
A program may use at most 64 MiB of HBM per device.

```python
import math
import jax
import jax.numpy as jnp
from jax import lax

CHANNELS = 3
TEMPLATE_LEN = 150
TEMPLATES = 512
MAXMO = 256
STATIONS = 32
NT = 1024


def set_ends(entries, key, least, largest):
    place = [jax.random.randint(jax.random.fold_in(key, axis), (), 0, length) for axis, length in enumerate(entries.shape)]
    main_axis = entries.shape.index(max(entries.shape))
    next_to = place[:main_axis] + [(place[main_axis] + 1) % entries.shape[main_axis]] + place[main_axis + 1:]
    return entries.at[tuple(place)].set(least).at[tuple(next_to)].set(largest)


def level_of(key, extent, split, low, high):
    def one(position, shards_of):
        steps = jax.random.uniform(jax.random.fold_in(jax.random.fold_in(key, 6), position), (shards_of,), jnp.float32, low / len(split), high / len(split))
        return jnp.repeat(jnp.exp(steps), extent[position] // shards_of).reshape((-1,) + (1,) * (len(extent) - position - 1))

    gain = one(*split[0])
    for cut in split[1:]:
        gain = gain * one(*cut)
    return gain


def normal_values(rng, shape, scale, most, split=(), held_as=jnp.bfloat16):
    array = scale * jax.random.normal(rng, shape, jnp.float32)
    if split:
        array = array * level_of(rng, shape, split, -0.22, 0.18)
    return jnp.clip(array, -most, most).astype(held_as)


def setup_inputs(seed: int = 0) -> dict:
    keys = jax.random.split(jax.random.key(seed), 6)
    return {
        "records": normal_values(keys[0], (STATIONS, CHANNELS, NT), 1.0, 6.0, ((0, 16), (2, 2))),
        "templates": normal_values(keys[1], (TEMPLATES, STATIONS, CHANNELS, TEMPLATE_LEN), 1.0, 6.0, ((1, 16),)),
        "moveout": set_ends(jax.random.randint(keys[2], (TEMPLATES, STATIONS), 0, MAXMO + 1), jax.random.fold_in(keys[2], 1), 0, MAXMO).astype(jnp.int32),
        "gap_start": set_ends(jax.random.randint(keys[3], (STATIONS, CHANNELS), 0, NT), jax.random.fold_in(keys[3], 1), 0, NT - 1).astype(jnp.int32),
        "gap_length": set_ends(jax.random.randint(keys[4], (STATIONS, CHANNELS), 0, 4 * TEMPLATE_LEN), jax.random.fold_in(keys[4], 1), 0, (4 * TEMPLATE_LEN) - 1).astype(jnp.int32),
    }


def hankel(extended, full_width):
    return jnp.stack([extended[..., offset:offset + full_width] for offset in range(TEMPLATE_LEN)], axis=-2)

def whiten(extended, full_width):
    widened = hankel(extended, full_width).astype(jnp.float32)
    energy = lax.optimization_barrier(jnp.sum(widened * widened, axis=-2, keepdims=True))
    return (widened / jnp.sqrt(jnp.maximum(energy, 1.0))).astype(jnp.bfloat16)

def unit_templates(templates):
    widened = templates.astype(jnp.float32)
    return (widened / jnp.sqrt(lax.optimization_barrier(jnp.sum(widened * widened, axis=-1, keepdims=True)) + 1e-06)).astype(jnp.bfloat16)

def gap_mask(positions, gap_start, gap_length):
    first = gap_start[..., None]
    return (positions < first) | (positions >= first + gap_length[..., None])

def reference(records, templates, moveout, gap_start, gap_length):
    total_len = records.shape[-1]
    halo_width = MAXMO + TEMPLATE_LEN - 1
    extended = jnp.pad(records, ((0, 0), (0, 0), (0, halo_width)))
    positions = jnp.arange(total_len + halo_width, dtype=jnp.int32)
    kept_mask = gap_mask(positions, gap_start, gap_length)
    extended = jnp.where(kept_mask, extended, jnp.zeros_like(extended))
    full_width = total_len + MAXMO
    normed = unit_templates(templates)
    columns = jnp.arange(total_len, dtype=jnp.int32)

    def station_step(running, inputs):
        station_data, weights, lag_rows = inputs
        lagged = whiten(station_data, full_width).reshape(CHANNELS * TEMPLATE_LEN, full_width)
        weight_rows = weights.reshape(weights.shape[0], CHANNELS * TEMPLATE_LEN)
        correlation = jnp.dot(weight_rows, lagged, preferred_element_type=jnp.float32)
        shifted = jnp.take_along_axis(correlation, lag_rows[:, None] + columns[None, :], axis=1)
        return (running + shifted, None)
    initial = jnp.zeros((TEMPLATES, total_len), jnp.float32)
    stacked, _ = lax.scan(station_step, initial, (extended, jnp.swapaxes(normed, 0, 1), moveout.T))
    return stacked * math.sqrt(TEMPLATE_LEN / (3.0 * STATIONS))
```

```python
import functools
import math

import jax
import jax.numpy as jnp
from jax import lax
from jax.experimental import pallas as pl
from jax.experimental.pallas import tpu as pltpu
from jax.sharding import PartitionSpec as P

CHANNELS = 3
TEMPLATE_LEN = 150
MAXMO = 256
LANES = 128
PADDED = -(-TEMPLATE_LEN // 16) * 16

f32, bf16, i32 = jnp.float32, jnp.bfloat16, jnp.int32


def unit_kernel(raw, unit, apart):
    stations = raw.shape[2]
    for c in range(CHANNELS):
        for j in range(raw.shape[3] // LANES):
            lanes = pl.ds(j * LANES, LANES)
            apart[j] = raw[c, :, :, lanes].astype(f32).reshape(TEMPLATE_LEN * stations, LANES)
            for s in range(stations):
                wave = apart[j, pl.ds(s, TEMPLATE_LEN, stride=stations), :]
                norm = lax.rsqrt(jnp.sum(wave * wave, axis=0, keepdims=True) + 1e-6)
                unit[s, pl.ds(c * PADDED, TEMPLATE_LEN), lanes] = (wave * norm).astype(bf16)
                unit[s, pl.ds(c * PADDED + TEMPLATE_LEN, PADDED - TEMPLATE_LEN), lanes] = jnp.zeros(
                    (PADDED - TEMPLATE_LEN, LANES), bf16
                )


def left(rows, by):
    return rows if by == 0 else pltpu.roll(rows, rows.shape[1] - by, 1)


def mask_and_energy(own, following, first_sample, gap_start, gap_length, rows, staggered, inverse):
    width = own.shape[2]
    stations = own.shape[1]
    full = inverse.shape[1]
    for c in range(CHANNELS):
        at = pl.ds(c * stations, stations)
        rows[at, pl.ds(0, width)] = own[c].astype(f32)
        rows[at, pl.ds(width, width)] = following[c].astype(f32)
    count = rows.shape[0]
    row = lax.broadcasted_iota(i32, (count, 1), 0)
    first = jnp.zeros((count, 1), i32)
    length = jnp.zeros((count, 1), i32)
    for c in range(CHANNELS):
        for s in range(stations):
            here = row == c * stations + s
            first = jnp.where(here, gap_start[s, c], first)
            length = jnp.where(here, gap_length[s, c], length)
    position = first_sample[0] + lax.broadcasted_iota(i32, (count, 2 * width), 1)
    kept = (position < first) | (position >= first + length)
    masked = jnp.where(kept, rows[...], 0.0)
    power, energy, offset, span = masked * masked, None, 0, 1
    while span <= TEMPLATE_LEN:
        if TEMPLATE_LEN & span:
            term = left(power, offset)
            energy = term if energy is None else energy + term
            offset += span
        power = power + left(power, span)
        span *= 2
    inverse[...] = lax.rsqrt(jnp.maximum(energy[:, :full], 1.0))
    for r in range(8):
        moved = left(masked, r)
        for j in range(staggered.shape[0]):
            staggered[j, pl.ds(r, count, stride=8), :] = moved[:, j * LANES : (j + 1) * LANES]


def lag_matrix(staggered, inverse, lagged):
    stations, _, full = lagged.shape
    for s in range(stations):
        for c in range(CHANNELS):
            r = c * stations + s
            eight = jnp.concatenate(
                [staggered[j, pl.ds(8 * r, 8), :] for j in range(staggered.shape[0])], axis=1
            )
            scale = jnp.broadcast_to(inverse[pl.ds(r, 1), :], (8, full))
            for q in range(0, PADDED, 16):
                upper = eight[:, q : q + full] * scale
                lower = eight[:, q + 8 : q + 8 + full] * scale
                lagged[s, pl.ds(c * PADDED + q, 16), :] = jnp.concatenate(
                    [upper, lower], axis=0
                ).astype(bf16)


def shifted(correlation, lags, s, start, count, width):
    tiles = width // LANES
    at = pl.ds(start, count)
    v = [correlation[s, at, pl.ds(j * LANES, LANES)] for j in range(tiles + MAXMO // LANES)]
    lag = jnp.broadcast_to(lags[at, s : s + 1], (count, LANES))
    none, one = lag < LANES, lag < 2 * LANES
    reach = lax.broadcasted_iota(i32, (count, LANES), 1) + lax.rem(lag, LANES)
    within = reach < LANES
    lane = lax.rem(reach, LANES)
    whole = [
        jnp.where(none, v[j], jnp.where(one, v[j + 1], v[min(j + 2, tiles + 1)]))
        for j in range(tiles + 1)
    ]
    fine = [jnp.take_along_axis(t, lane, axis=1, mode="promise_in_bounds") for t in whole]
    return [jnp.where(within, fine[j], fine[j + 1]) for j in range(tiles)]


def stack_kernel(
    own, following, first_sample, gap_start, gap_length, moveout, unit, stack,
    rows, staggered, inverse, lagged, lag_rows, lags, correlation,
):
    stations, templates = moveout.shape
    width = own.shape[2]
    mask_and_energy(own, following, first_sample, gap_start, gap_length, rows, staggered, inverse)
    lag_matrix(staggered, inverse, lagged)
    lag_rows[pl.ds(0, stations), :] = moveout[...].astype(f32)
    for k in range(0, templates, LANES):
        lags[pl.ds(k, LANES), :] = lag_rows[:, pl.ds(k, LANES)].T.astype(i32)
    for s in range(stations):
        correlation[s] = lax.dot_general(
            unit[s], lagged[s], (((0,), (0,)), ((), ())), preferred_element_type=f32
        )
    count = 16

    def block(i, _):
        start = pl.multiple_of(i * count, count)
        total = shifted(correlation, lags, 0, start, count, width)
        for s in range(1, stations):
            total = [a + b for a, b in zip(total, shifted(correlation, lags, s, start, count, width))]
        stack[pl.ds(start, count), :] = jnp.concatenate(total, axis=1).astype(bf16)
        return 0

    lax.fori_loop(0, templates // count, block, 0, unroll=4)


def shards(records, templates, moveout, gap_start, gap_length):
    stations, _, width = records.shape
    number = templates.shape[0]
    full = width + MAXMO
    devices = lax.axis_size("tm")
    own = records.transpose(1, 0, 2)
    following = lax.ppermute(own, "tm", [(i, i - 1) for i in range(1, devices)])
    vmem = pl.BlockSpec(memory_space=pltpu.VMEM)
    smem = pl.BlockSpec(memory_space=pltpu.SMEM)
    params = pltpu.CompilerParams(vmem_limit_bytes=48 * 1024 * 1024)
    depth = CHANNELS * PADDED
    unit = pl.pallas_call(
        unit_kernel,
        out_shape=jax.ShapeDtypeStruct((stations, depth, number), bf16),
        in_specs=[vmem],
        out_specs=vmem,
        scratch_shapes=[pltpu.VMEM((number // LANES, TEMPLATE_LEN * stations, LANES), f32)],
        compiler_params=params,
        cost_estimate=pl.CostEstimate(flops=10**9, bytes_accessed=2 * 10**6, transcendentals=0),
    )(templates.transpose(2, 3, 1, 0))
    first_sample = (lax.axis_index("tm") * width).astype(i32).reshape(1)
    stack = pl.pallas_call(
        stack_kernel,
        out_shape=jax.ShapeDtypeStruct((number, width), bf16),
        in_specs=[vmem, vmem, smem, smem, smem, vmem, vmem],
        out_specs=vmem,
        scratch_shapes=[
            pltpu.VMEM((8, 2 * width), f32),
            pltpu.VMEM((2 * width // LANES, 64, LANES), f32),
            pltpu.VMEM((8, full), f32),
            pltpu.VMEM((stations, depth, full), bf16),
            pltpu.VMEM((8, number), f32),
            pltpu.VMEM((number, 8), i32),
            pltpu.VMEM((stations, number, full), f32),
        ],
        compiler_params=params,
        cost_estimate=pl.CostEstimate(flops=2 * 10**9, bytes_accessed=2 * 10**6, transcendentals=0),
    )(own, following, first_sample, gap_start, gap_length, moveout.T, unit)
    groups = lax.axis_size("sta")
    parts = lax.all_to_all(stack, "sta", 0, 0, tiled=True).reshape(groups, number // groups, width)
    return jnp.sum(parts.astype(f32), axis=0) * math.sqrt(TEMPLATE_LEN / (3.0 * stations * groups))


def solution(mesh):
    placed = (
        P("sta", None, "tm"),
        P(None, "sta", None, None),
        P(None, "sta"),
        P("sta", None),
        P("sta", None),
    )
    return jax.shard_map(
        shards, mesh=mesh, in_specs=placed, out_specs=P("sta", "tm"), check_vma=False
    )
```

```python
import functools
import math

import jax
import jax.numpy as jnp
from jax import lax
from jax.experimental import pallas as pl
from jax.experimental.pallas import tpu as pltpu
from jax.sharding import PartitionSpec as P

CHANNELS = 3
TEMPLATE_LEN = 150
MAXMO = 256
FACTORS = (5, 5, 3, 2)
LANES = 128
PADDED = -(-TEMPLATE_LEN // 16) * 16

STEP = 16

f32, bf16, i32 = jnp.float32, jnp.bfloat16, jnp.int32


def setup_kernel(
    raw_hbm, moveout_hbm, gap_start_hbm, gap_length_hbm, own_hbm,
    unit, lags, kept, masked,
    raw, moveout, gap_start, gap_length, own, apart, tall, lag_rows, rows, sems,
):
    stations, templates = moveout.shape
    width = own.shape[2]
    copies = [pltpu.make_async_copy(raw_hbm.at[c], raw.at[c], sems.at[c]) for c in range(CHANNELS)]
    small = [(moveout_hbm, moveout), (gap_start_hbm, gap_start), (gap_length_hbm, gap_length), (own_hbm, own)]
    small = [pltpu.make_async_copy(a, b, sems.at[CHANNELS + i]) for i, (a, b) in enumerate(small)]
    for copy in small + copies:
        copy.start()
    for copy in small:
        copy.wait()
    lag_rows[...] = jnp.zeros_like(lag_rows)
    lag_rows[pl.ds(0, stations), :] = moveout[...].astype(f32)
    for k in range(0, templates, LANES):
        columns = lag_rows[:, pl.ds(k, LANES)].T
        for s in range(stations):
            lags[s, pl.ds(k, LANES), :] = jnp.broadcast_to(columns[:, s : s + 1], (LANES, LANES)).astype(i32)
    count = rows.shape[0]
    row = lax.broadcasted_iota(i32, (count, 1), 0)
    first = jnp.zeros((count, 1), i32)
    length = jnp.zeros((count, 1), i32)
    rows[...] = jnp.zeros_like(rows)
    for c in range(CHANNELS):
        rows[pl.ds(c * stations, stations), :] = own[c].astype(f32)
        for s in range(stations):
            here = row == c * stations + s
            first = jnp.where(here, gap_start[s, c], first)
            length = jnp.where(here, gap_length[s, c], length)
    position = lax.axis_index("tm") * width + lax.broadcasted_iota(i32, (count, 2 * width), 1)
    keep = ((position < first) | (position >= first + length)) & (position < lax.axis_size("tm") * width)
    kept[...] = jnp.where(keep[:, width:], 1.0, 0.0)
    masked[...] = jnp.where(keep[:, :width], rows[...], 0.0)
    tall[...] = jnp.zeros_like(tall)
    groups = templates // LANES
    for c in range(CHANNELS):
        copies[c].wait()
        apart[...] = raw[c].astype(f32)
        for j in range(groups):
            for s in range(stations):
                wave = apart[pl.ds(j * stations + s, TEMPLATE_LEN, stride=groups * stations), :]
                norm = lax.rsqrt(jnp.sum(wave * wave, axis=0, keepdims=True) + 1e-6)
                tall[s, j, pl.ds(c * PADDED, TEMPLATE_LEN), :] = (wave * norm).astype(bf16)
    for s in range(stations):
        for j in range(templates // LANES):
            unit[s, pl.ds(j * LANES, LANES), :] = tall[s, j].T


def left(rows, by):
    return rows if by == 0 else pltpu.roll(rows, rows.shape[1] - by, 1)


def lag_matrix(masked, kept, following, staggered, inverse, lagged):
    stations, _, full = lagged.shape
    count, width = masked.shape
    beyond = [jnp.zeros((count - CHANNELS * stations, width), f32)]
    after = jnp.concatenate([following[c].astype(f32) for c in range(CHANNELS)] + beyond, axis=0)
    samples = jnp.concatenate([masked[...], jnp.where(kept[...] > 0.5, after, 0.0)], axis=1)
    energy, span = samples * samples, 1
    for factor in FACTORS:
        energy = sum((left(energy, i * span) for i in range(1, factor)), energy)
        span *= factor
    inverse[...] = lax.rsqrt(jnp.maximum(energy[:, :full], 1.0))
    for r in range(STEP):
        moved = left(samples, r)
        for j in range(staggered.shape[0]):
            staggered[j, pl.ds(r, count, stride=STEP), :] = moved[:, j * LANES : (j + 1) * LANES]
    lane = lax.broadcasted_iota(i32, (STEP, LANES), 1)
    for s in range(stations):
        for c in range(CHANNELS):
            r = c * stations + s
            tiles = [
                staggered[j, pl.ds(STEP * r, STEP), :].astype(bf16) for j in range(staggered.shape[0])
            ]
            scale = [
                jnp.broadcast_to(inverse[pl.ds(r, 1), pl.ds(j * LANES, LANES)], (STEP, LANES))
                for j in range(full // LANES)
            ]
            for turn in range(0, min(PADDED, LANES), STEP):
                turned = [pltpu.roll(t, LANES - turn, 1) if turn else t for t in tiles]
                near = [
                    jnp.where(lane < LANES - turn, x, y) if turn else x
                    for x, y in zip(turned, turned[1:] + turned[:1])
                ]
                for q in range(turn, PADDED, LANES):
                    for j in range(full // LANES):
                        lagged[s, pl.ds(c * PADDED + q, STEP), pl.ds(j * LANES, LANES)] = (
                            near[j + q // LANES].astype(f32) * scale[j]
                        ).astype(bf16)


def shifted(correlation, lags, s, row, template, count, width):
    tiles = width // LANES
    at = pl.ds(row, count)
    v = [correlation[s, at, pl.ds(j * LANES, LANES)] for j in range(tiles + MAXMO // LANES)]
    lag = lags[s, pl.ds(template, count), :]
    none, one = lag < LANES, lag < 2 * LANES
    reach = lax.broadcasted_iota(i32, (count, LANES), 1) + (lag & (LANES - 1))
    within = reach < LANES
    lane = reach & (LANES - 1)
    whole = [
        jnp.where(none, v[j], jnp.where(one, v[j + 1], v[min(j + 2, tiles + 1)]))
        for j in range(tiles + 1)
    ]
    fine = [jnp.take_along_axis(t, lane, axis=1, mode="promise_in_bounds") for t in whole]
    return [jnp.where(within, fine[j], fine[j + 1]) for j in range(tiles)]


def stack_rows(correlation, lags, first, templates_of, target, scale):
    stations = correlation.shape[0]
    width = target.shape[1]
    count = 16

    def block(i, _):
        to = pl.multiple_of(i * count, count)
        template = pl.multiple_of(templates_of(i), count)
        total = shifted(correlation, lags, 0, first + to, template, count, width)
        for s in range(1, stations):
            more = shifted(correlation, lags, s, first + to, template, count, width)
            total = [a + b for a, b in zip(total, more)]
        for j, t in enumerate(total):
            target[pl.ds(to, count), pl.ds(j * LANES, LANES)] = (t * scale).astype(target.dtype)
        return 0

    lax.fori_loop(0, target.shape[0] // count, block, 0, unroll=8)


def place():
    me = lax.axis_index("sta")
    return me & 1, (me >> 1) & 1, me >> 2


def rows_of(owned, block_of):
    per = owned // 16
    return lambda i: block_of(i // per) * owned + i % per * 16


def correlate(owned, unit, lagged, block_of, correlation):
    for s in range(unit.shape[0]):
        blocks = [
            unit[s, pl.ds(pl.multiple_of(block_of(b) * owned, 16), owned), :]
            for b in range(correlation.shape[1] // owned)
        ]
        correlation[s] = jnp.dot(
            jnp.concatenate(blocks, axis=0), lagged[s], preferred_element_type=f32
        )


def owners(rest, across):
    core, pair, _ = place()
    return lambda b: (b % rest * 2 + (pair ^ across)) * 2 + (core ^ 1 ^ (b // rest))


def first_kernel(
    owned, scale, masked, kept, following, unit, lags, lagged, correlation, away, staggered, inverse,
):
    lag_matrix(masked, kept, following, staggered, inverse, lagged)
    block_of = owners(away.shape[0] // owned, 1)
    correlate(owned, unit, lagged, block_of, correlation)
    stack_rows(correlation, lags, 0, rows_of(owned, block_of), away, scale)


def second_kernel(owned, scale, lagged, unit, lags, correlation, away):
    block_of = owners(away.shape[0] // owned, 0)
    correlate(owned, unit, lagged, block_of, correlation)
    stack_rows(correlation, lags, 0, rows_of(owned, block_of), away, scale)


def home_kernel(owned, scale, across, correlation, lags, target):
    rest = target.shape[0] // owned
    block_of = owners(rest, across)
    stack_rows(
        correlation, lags, target.shape[0], rows_of(owned, lambda b: block_of(b + rest)), target, scale
    )


def split_kernel(home, core, pair, own, *others):
    owned = own.shape[0]
    _, _, rest = place()
    for k, target in enumerate((own,) + others):
        at = pl.ds(pl.multiple_of((rest ^ k) * owned, 16), owned)
        total = home[at, :] + core[at, :].astype(f32) + pair[at, :].astype(f32)
        target[...] = total.astype(target.dtype)


def shards(records, templates, moveout, gap_start, gap_length):
    stations, _, width = records.shape
    number = templates.shape[0]
    full = width + MAXMO
    devices = lax.axis_size("tm")
    groups = lax.axis_size("sta")
    owned = number // groups
    rest = groups // 4
    scale = math.sqrt(TEMPLATE_LEN / (3.0 * stations * groups))
    own = records.transpose(1, 0, 2)
    following = lax.ppermute(own, "tm", [(i, (i - 1) % devices) for i in range(devices)])
    vmem = pl.BlockSpec(memory_space=pltpu.VMEM)
    hbm = pl.BlockSpec(memory_space=pltpu.HBM)
    depth = CHANNELS * PADDED

    def call(kernel, outs, ins, scratch=(), flops=10**9):
        return pl.pallas_call(
            kernel,
            out_shape=tuple(jax.ShapeDtypeStruct(shape, dtype) for shape, dtype in outs),
            in_specs=ins,
            out_specs=tuple(vmem for _ in outs),
            scratch_shapes=scratch,
            compiler_params=pltpu.CompilerParams(vmem_limit_bytes=24 * 1024 * 1024),
            cost_estimate=pl.CostEstimate(flops=flops, bytes_accessed=2 * 10**6, transcendentals=0),
        )

    flat = templates.transpose(2, 3, 1, 0).reshape(CHANNELS, TEMPLATE_LEN, stations, number // LANES, LANES)
    flat = flat.transpose(0, 1, 3, 2, 4).reshape(CHANNELS, TEMPLATE_LEN * stations * number // LANES, LANES)
    unit, lags, kept, masked = call(
        setup_kernel,
        [
            ((stations, number, depth), bf16),
            ((stations, number, LANES), i32),
            ((8, width), f32),
            ((8, width), f32),
        ],
        [hbm] * 5,
        [
            pltpu.VMEM((CHANNELS, TEMPLATE_LEN * stations * number // LANES, LANES), bf16),
            pltpu.VMEM((stations, number), i32),
            pltpu.SMEM((stations, CHANNELS), i32),
            pltpu.SMEM((stations, CHANNELS), i32),
            pltpu.VMEM((CHANNELS, stations, width), bf16),
            pltpu.VMEM((TEMPLATE_LEN * stations * number // LANES, LANES), f32),
            pltpu.VMEM((stations, number // LANES, depth, LANES), bf16),
            pltpu.VMEM((8, number), f32),
            pltpu.VMEM((8, width), f32),
            pltpu.SemaphoreType.DMA((CHANNELS + 4,)),
        ],
    )(
        *(
            pltpu.with_memory_space_constraint(a, pltpu.HBM)
            for a in (flat, moveout.T, gap_start, gap_length, own)
        )
    )
    half = ((stations, number // 2, full), f32)
    quarter = (number // 4, width)
    lagged, correlation, away = call(
        functools.partial(first_kernel, owned, scale),
        [((stations, depth, full), bf16), half, (quarter, bf16)],
        [vmem] * 5,
        [
            pltpu.VMEM((2 * width // LANES, 8 * STEP, LANES), f32),
            pltpu.VMEM((8, full), f32),
        ],
    )(masked, kept, following, unit, lags)

    def exchange(value, bit):
        return lax.ppermute(value, "sta", [(i, i ^ bit) for i in range(groups)])

    from_core = exchange(away, 1)
    (to_pair,) = call(functools.partial(home_kernel, owned, scale, 1), [(quarter, f32)], [vmem] * 2)(correlation, lags)
    to_pair = (to_pair + from_core.astype(f32)).astype(bf16)
    from_pair = exchange(to_pair, 2)
    correlation, away = call(
        functools.partial(second_kernel, owned, scale), [half, (quarter, bf16)], [vmem] * 3
    )(lagged, unit, lags)
    from_core = exchange(away, 1)
    (home,) = call(functools.partial(home_kernel, owned, scale, 0), [(quarter, f32)], [vmem] * 2)(correlation, lags)
    mine, *others = call(
        split_kernel, [((owned, width), f32)] + [((owned, width), bf16)] * (rest - 1), [vmem] * 3
    )(home, from_core, from_pair)
    arrived = [exchange(others[k - 1], 4 * k) for k in range(rest - 1, 0, -1)]
    for part in arrived:
        mine = mine + part.astype(f32)
    return mine


def solution(mesh):
    placed = (
        P("sta", None, "tm"),
        P(None, "sta", None, None),
        P(None, "sta"),
        P("sta", None),
        P("sta", None),
    )
    return jax.shard_map(
        shards, mesh=mesh, in_specs=placed, out_specs=P("sta", "tm"), check_vma=False
    )
```

```python
import functools
import math

import jax
import jax.numpy as jnp
from jax import lax
from jax.experimental import pallas as pl
from jax.experimental.pallas import tpu as pltpu
from jax.sharding import PartitionSpec as P

CHANNELS = 3
TEMPLATE_LEN = 150
MAXMO = 256
FACTORS = (5, 5, 3, 2)
LANES = 128
PADDED = -(-TEMPLATE_LEN // 16) * 16

STEP = 16

f32, bf16, i32 = jnp.float32, jnp.bfloat16, jnp.int32


def setup_kernel(
    raw_hbm, moveout_hbm, gap_start_hbm, gap_length_hbm, own_hbm,
    unit, lags, kept, masked,
    raw, moveout, gap_start, gap_length, own, apart, tall, lag_rows, rows, sems,
):
    stations, templates = moveout.shape
    width = own.shape[2]
    copies = [pltpu.make_async_copy(raw_hbm.at[c], raw.at[c], sems.at[c]) for c in range(CHANNELS)]
    small = [(moveout_hbm, moveout), (gap_start_hbm, gap_start), (gap_length_hbm, gap_length), (own_hbm, own)]
    small = [pltpu.make_async_copy(a, b, sems.at[CHANNELS + i]) for i, (a, b) in enumerate(small)]
    for copy in small + copies:
        copy.start()
    for copy in small:
        copy.wait()
    count = rows.shape[0]
    row = lax.broadcasted_iota(i32, (count, 1), 0)
    first = jnp.zeros((count, 1), i32)
    length = jnp.zeros((count, 1), i32)
    rows[...] = jnp.zeros_like(rows)
    for c in range(CHANNELS):
        rows[pl.ds(c * stations, stations), :] = own[c].astype(f32)
        for s in range(stations):
            here = row == c * stations + s
            first = jnp.where(here, gap_start[s, c], first)
            length = jnp.where(here, gap_length[s, c], length)
    position = lax.axis_index("tm") * width + lax.broadcasted_iota(i32, (count, 2 * width), 1)
    keep = ((position < first) | (position >= first + length)) & (position < lax.axis_size("tm") * width)
    kept[...] = jnp.where(keep[:, width:], 1.0, 0.0)
    masked[...] = jnp.where(keep[:, :width], rows[...], 0.0)
    groups = templates // LANES
    for c in range(CHANNELS):
        copies[c].wait()
        if c == 0:
            lag_rows[...] = jnp.zeros_like(lag_rows)
            lag_rows[pl.ds(0, stations), :] = moveout[...].astype(f32)
            for k in range(0, templates, LANES):
                columns = lag_rows[:, pl.ds(k, LANES)].T
                for s in range(stations):
                    lags[s, pl.ds(k, LANES), :] = jnp.broadcast_to(columns[:, s : s + 1], (LANES, LANES)).astype(i32)
        apart[...] = raw[c].astype(f32)
        for j in range(groups):
            for s in range(stations):
                wave = apart[pl.ds(j * stations + s, TEMPLATE_LEN, stride=groups * stations), :]
                norm = lax.rsqrt(jnp.sum(wave * wave, axis=0, keepdims=True) + 1e-6)
                wave = jnp.concatenate([wave * norm, jnp.zeros((PADDED - TEMPLATE_LEN, LANES), f32)], axis=0)
                tall[s, j, pl.ds(c * PADDED, PADDED), :] = wave.astype(bf16)
    for s in range(stations):
        for j in range(templates // LANES):
            unit[s, pl.ds(j * LANES, LANES), :] = tall[s, j].T


def left(rows, by):
    return rows if by == 0 else pltpu.roll(rows, rows.shape[1] - by, 1)


def lag_matrix(masked, kept, following, staggered, inverse, lagged):
    stations, _, full = lagged.shape
    count, width = masked.shape
    beyond = [jnp.zeros((count - CHANNELS * stations, width), f32)]
    after = jnp.concatenate([following[c].astype(f32) for c in range(CHANNELS)] + beyond, axis=0)
    samples = jnp.concatenate([masked[...], jnp.where(kept[...] > 0.5, after, 0.0)], axis=1)
    energy, span = samples * samples, 1
    for factor in FACTORS:
        energy = sum((left(energy, i * span) for i in range(1, factor)), energy)
        span *= factor
    inverse[...] = lax.rsqrt(jnp.maximum(energy[:, :full], 1.0))
    for r in range(STEP):
        moved = left(samples, r)
        for j in range(staggered.shape[0]):
            staggered[j, pl.ds(r, count, stride=STEP), :] = moved[:, j * LANES : (j + 1) * LANES]
    lane = lax.broadcasted_iota(i32, (STEP, LANES), 1)
    for s in range(stations):
        for c in range(CHANNELS):
            r = c * stations + s
            tiles = [
                staggered[j, pl.ds(STEP * r, STEP), :].astype(bf16) for j in range(staggered.shape[0])
            ]
            scale = [
                jnp.broadcast_to(inverse[pl.ds(r, 1), pl.ds(j * LANES, LANES)], (STEP, LANES))
                for j in range(full // LANES)
            ]
            for turn in range(0, min(PADDED, LANES), STEP):
                turned = [pltpu.roll(t, LANES - turn, 1) if turn else t for t in tiles]
                near = [
                    jnp.where(lane < LANES - turn, x, y) if turn else x
                    for x, y in zip(turned, turned[1:] + turned[:1])
                ]
                for q in range(turn, PADDED, LANES):
                    for j in range(full // LANES):
                        lagged[s, pl.ds(c * PADDED + q, STEP), pl.ds(j * LANES, LANES)] = (
                            near[j + q // LANES].astype(f32) * scale[j]
                        ).astype(bf16)


def shifted(correlation, lags, s, row, template, count, width):
    tiles = width // LANES
    at = pl.ds(row, count)
    v = [correlation[s, at, pl.ds(j * LANES, LANES)] for j in range(tiles + MAXMO // LANES)]
    lag = lags[s, pl.ds(template, count), :]
    none, one = lag < LANES, lag < 2 * LANES
    reach = lax.broadcasted_iota(i32, (count, LANES), 1) + (lag & (LANES - 1))
    within = reach < LANES
    lane = reach & (LANES - 1)
    whole = [
        jnp.where(none, v[j], jnp.where(one, v[j + 1], v[min(j + 2, tiles + 1)]))
        for j in range(tiles + 1)
    ]
    fine = [jnp.take_along_axis(t, lane, axis=1, mode="promise_in_bounds") for t in whole]
    return [jnp.where(within, fine[j], fine[j + 1]) for j in range(tiles)]


def stack_rows(correlation, lags, first, templates_of, target, scale):
    stations = correlation.shape[0]
    width = target.shape[1]
    count = 16

    def block(i, _):
        to = pl.multiple_of(i * count, count)
        template = pl.multiple_of(templates_of(i), count)
        total = shifted(correlation, lags, 0, first + to, template, count, width)
        for s in range(1, stations):
            more = shifted(correlation, lags, s, first + to, template, count, width)
            total = [a + b for a, b in zip(total, more)]
        for j, t in enumerate(total):
            target[pl.ds(to, count), pl.ds(j * LANES, LANES)] = (t * scale).astype(target.dtype)
        return 0

    lax.fori_loop(0, target.shape[0] // count, block, 0, unroll=8)


def place():
    me = lax.axis_index("sta")
    return me & 1, (me >> 1) & 1, me >> 2


def rows_of(owned, block_of):
    per = owned // 16
    return lambda i: block_of(i // per) * owned + i % per * 16


def correlate(owned, unit, lagged, block_of, correlation):
    for s in range(unit.shape[0]):
        blocks = [
            unit[s, pl.ds(pl.multiple_of(block_of(b) * owned, 16), owned), :]
            for b in range(correlation.shape[1] // owned)
        ]
        correlation[s] = jnp.dot(
            jnp.concatenate(blocks, axis=0), lagged[s], preferred_element_type=f32
        )


def quarter_kernel(owned, scale, other_pair, other_core, lagged, unit, lags, target, correlation):
    core, pair, rest = place()
    block_of = lambda b: ((rest ^ b) * 2 + (pair ^ other_pair)) * 2 + (core ^ other_core)
    correlate(owned, unit, lagged, block_of, correlation)
    stack_rows(correlation, lags, 0, rows_of(owned, block_of), target, scale)


def first_kernel(
    owned, scale, masked, kept, following, unit, lags, lagged, away, correlation, staggered, inverse,
):
    lag_matrix(masked, kept, following, staggered, inverse, lagged)
    quarter_kernel(owned, scale, 1, 1, lagged, unit, lags, away, correlation)


def sum_kernel(first, home, core, pair, *targets):
    for k, target in enumerate(targets):
        owned = target.shape[0]
        here, there = pl.ds((first + k) * owned, owned), pl.ds(k * owned, owned)
        total = home[here, :] + core[here, :].astype(f32) + pair[there, :].astype(f32)
        target[...] = total.astype(target.dtype)


def shards(records, templates, moveout, gap_start, gap_length):
    stations, _, width = records.shape
    number = templates.shape[0]
    full = width + MAXMO
    devices = lax.axis_size("tm")
    groups = lax.axis_size("sta")
    owned = number // groups
    rest = groups // 4
    scale = math.sqrt(TEMPLATE_LEN / (3.0 * stations * groups))
    own = records.transpose(1, 0, 2)
    following = lax.ppermute(own, "tm", [(i, (i - 1) % devices) for i in range(devices)])
    vmem = pl.BlockSpec(memory_space=pltpu.VMEM)
    hbm = pl.BlockSpec(memory_space=pltpu.HBM)
    depth = CHANNELS * PADDED

    def call(kernel, outs, ins, scratch=(), flops=10**9):
        return pl.pallas_call(
            kernel,
            out_shape=tuple(jax.ShapeDtypeStruct(shape, dtype) for shape, dtype in outs),
            in_specs=ins,
            out_specs=tuple(vmem for _ in outs),
            scratch_shapes=scratch,
            compiler_params=pltpu.CompilerParams(vmem_limit_bytes=24 * 1024 * 1024),
            cost_estimate=pl.CostEstimate(flops=flops, bytes_accessed=2 * 10**6, transcendentals=0),
        )

    flat = templates.transpose(2, 3, 1, 0).reshape(CHANNELS, TEMPLATE_LEN, stations, number // LANES, LANES)
    flat = flat.transpose(0, 1, 3, 2, 4).reshape(CHANNELS, TEMPLATE_LEN * stations * number // LANES, LANES)
    unit, lags, kept, masked = call(
        setup_kernel,
        [
            ((stations, number, depth), bf16),
            ((stations, number, LANES), i32),
            ((8, width), f32),
            ((8, width), f32),
        ],
        [hbm] * 5,
        [
            pltpu.VMEM((CHANNELS, TEMPLATE_LEN * stations * number // LANES, LANES), bf16),
            pltpu.VMEM((stations, number), i32),
            pltpu.SMEM((stations, CHANNELS), i32),
            pltpu.SMEM((stations, CHANNELS), i32),
            pltpu.VMEM((CHANNELS, stations, width), bf16),
            pltpu.VMEM((TEMPLATE_LEN * stations * number // LANES, LANES), f32),
            pltpu.VMEM((stations, number // LANES, depth, LANES), bf16),
            pltpu.VMEM((8, number), f32),
            pltpu.VMEM((8, width), f32),
            pltpu.SemaphoreType.DMA((CHANNELS + 4,)),
        ],
    )(
        *(
            pltpu.with_memory_space_constraint(a, pltpu.HBM)
            for a in (flat, moveout.T, gap_start, gap_length, own)
        )
    )
    quarter = (number // 4, width)
    columns = pltpu.VMEM((stations, number // 4, full), f32)
    lagged, away = call(
        functools.partial(first_kernel, owned, scale),
        [((stations, depth, full), bf16), (quarter, bf16)],
        [vmem] * 5,
        [columns, pltpu.VMEM((2 * width // LANES, 8 * STEP, LANES), f32), pltpu.VMEM((8, full), f32)],
    )(masked, kept, following, unit, lags)

    def exchange(value, bit):
        return lax.ppermute(value, "sta", [(i, i ^ bit) for i in range(groups)])

    def stacked(other_pair, other_core, dtype):
        kernel = functools.partial(quarter_kernel, owned, scale, other_pair, other_core)
        return call(kernel, [(quarter, dtype)], [vmem] * 3, [columns])(lagged, unit, lags)[0]

    from_core = exchange(away, 1)
    to_pair = stacked(1, 0, f32)
    far = rest - 1
    at = far * owned
    from_far = exchange((to_pair[at:] + from_core[at:].astype(f32)).astype(bf16), 2)
    from_near = exchange((to_pair[:at] + from_core[:at].astype(f32)).astype(bf16), 2)
    away = stacked(0, 1, bf16)
    from_core = exchange(away, 1)
    home = stacked(0, 0, f32)
    block = (owned, width)
    fars = call(
        functools.partial(sum_kernel, far), [(block, bf16)] * (rest - far), [vmem] * 3
    )(home, from_core, from_far)
    arrived = [exchange(fars[k - far], 4 * k) for k in range(rest - 1, far - 1, -1)]
    mine, *nears = call(
        functools.partial(sum_kernel, 0), [(block, f32)] + [(block, bf16)] * (far - 1), [vmem] * 3
    )(home, from_core, from_near)
    arrived += [exchange(nears[k - 1], 4 * k) for k in range(far - 1, 0, -1)]
    for part in arrived:
        mine = mine + part.astype(f32)
    return mine


def solution(mesh):
    placed = (
        P("sta", None, "tm"),
        P(None, "sta", None, None),
        P(None, "sta"),
        P("sta", None),
        P("sta", None),
    )
    return jax.shard_map(
        shards, mesh=mesh, in_specs=placed, out_specs=P("sta", "tm"), check_vma=False
    )
```

```python
import functools
import math

import jax
import jax.numpy as jnp
from jax import lax
from jax.experimental import pallas as pl
from jax.experimental.pallas import tpu as pltpu
from jax.sharding import PartitionSpec as P

CHANNELS = 3
TEMPLATE_LEN = 150
MAXMO = 256
FACTORS = (5, 5, 3, 2)
LANES = 128
PADDED = -(-TEMPLATE_LEN // 16) * 16

PITCH = 17
STEP = 16

f32, bf16, i32 = jnp.float32, jnp.bfloat16, jnp.int32


def setup_kernel(
    raw_hbm, moveout_hbm, gap_start_hbm, gap_length_hbm, own_hbm,
    unit, lags, kept, masked,
    raw, moveout, gap_start, gap_length, own, apart, tall, lag_rows, rows, sems,
):
    stations, templates = moveout.shape
    width = own.shape[2]
    copies = [pltpu.make_async_copy(raw_hbm.at[c], raw.at[c], sems.at[c]) for c in range(CHANNELS)]
    small = [(moveout_hbm, moveout), (gap_start_hbm, gap_start), (gap_length_hbm, gap_length), (own_hbm, own)]
    small = [pltpu.make_async_copy(a, b, sems.at[CHANNELS + i]) for i, (a, b) in enumerate(small)]
    for copy in small + copies:
        copy.start()
    for copy in small:
        copy.wait()
    count = rows.shape[0]
    row = lax.broadcasted_iota(i32, (count, 1), 0)
    first = jnp.zeros((count, 1), i32)
    length = jnp.zeros((count, 1), i32)
    rows[...] = jnp.zeros_like(rows)
    for c in range(CHANNELS):
        rows[pl.ds(c * stations, stations), :] = own[c].astype(f32)
        for s in range(stations):
            here = row == c * stations + s
            first = jnp.where(here, gap_start[s, c], first)
            length = jnp.where(here, gap_length[s, c], length)
    position = lax.axis_index("tm") * width + lax.broadcasted_iota(i32, (count, 2 * width), 1)
    keep = ((position < first) | (position >= first + length)) & (position < lax.axis_size("tm") * width)
    kept[...] = jnp.where(keep[:, width:], 1.0, 0.0)
    masked[...] = jnp.where(keep[:, :width], rows[...], 0.0)
    groups = templates // LANES
    for c in range(CHANNELS):
        copies[c].wait()
        if c == 0:
            lag_rows[...] = jnp.zeros_like(lag_rows)
            lag_rows[pl.ds(0, stations), :] = moveout[...].astype(f32)
            for k in range(0, templates, LANES):
                columns = lag_rows[:, pl.ds(k, LANES)].T
                for s in range(stations):
                    lags[s, pl.ds(k, LANES), :] = jnp.broadcast_to(columns[:, s : s + 1], (LANES, LANES)).astype(i32)
        apart[...] = raw[c].astype(f32)
        for j in range(groups):
            for s in range(stations):
                wave = apart[pl.ds(j * stations + s, TEMPLATE_LEN, stride=groups * stations), :]
                norm = lax.rsqrt(jnp.sum(wave * wave, axis=0, keepdims=True) + 1e-6)
                wave = jnp.concatenate([wave * norm, jnp.zeros((PADDED - TEMPLATE_LEN, LANES), f32)], axis=0)
                tall[s, j, pl.ds(c * PADDED, PADDED), :] = wave.astype(bf16)
    for s in range(stations):
        for j in range(templates // LANES):
            unit[s, pl.ds(j * LANES, LANES), :] = tall[s, j].T


def left(rows, by):
    return rows if by == 0 else pltpu.roll(rows, rows.shape[1] - by, 1)


def lag_matrix(masked, kept, following, staggered, inverse, lagged):
    stations, _, full = lagged.shape
    count, width = masked.shape
    beyond = [jnp.zeros((count - CHANNELS * stations, width), f32)]
    after = jnp.concatenate([following[c].astype(f32) for c in range(CHANNELS)] + beyond, axis=0)
    samples = jnp.concatenate([masked[...], jnp.where(kept[...] > 0.5, after, 0.0)], axis=1)
    energy, span = samples * samples, 1
    for factor in FACTORS:
        energy = sum((left(energy, i * span) for i in range(1, factor)), energy)
        span *= factor
    inverse[...] = lax.rsqrt(jnp.maximum(energy[:, :full], 1.0))
    for r in range(STEP):
        moved = left(samples, r)
        for j in range(staggered.shape[0]):
            staggered[j, pl.ds(r, count, stride=PITCH), :] = moved[:, j * LANES : (j + 1) * LANES]
    lane = lax.broadcasted_iota(i32, (STEP, LANES), 1)
    for s in range(stations):
        for c in range(CHANNELS):
            r = c * stations + s
            tiles = [
                staggered[j, pl.ds(PITCH * r, STEP), :].astype(bf16) for j in range(staggered.shape[0])
            ]
            scale = [
                jnp.broadcast_to(inverse[pl.ds(r, 1), pl.ds(j * LANES, LANES)], (STEP, LANES))
                for j in range(full // LANES)
            ]
            for turn in range(0, min(PADDED, LANES), STEP):
                turned = [pltpu.roll(t, LANES - turn, 1) if turn else t for t in tiles]
                near = [
                    jnp.where(lane < LANES - turn, x, y) if turn else x
                    for x, y in zip(turned, turned[1:] + turned[:1])
                ]
                for q in range(turn, PADDED, LANES):
                    for j in range(full // LANES):
                        lagged[s, pl.ds(c * PADDED + q, STEP), pl.ds(j * LANES, LANES)] = (
                            near[j + q // LANES].astype(f32) * scale[j]
                        ).astype(bf16)


def shifted(correlation, lags, s, row, template, count, width):
    tiles = width // LANES
    at = pl.ds(row, count)
    v = [correlation[s, at, pl.ds(j * LANES, LANES)] for j in range(tiles + MAXMO // LANES)]
    lag = lags[s, pl.ds(template, count), :]
    none, one = lag < LANES, lag < 2 * LANES
    reach = lax.broadcasted_iota(i32, (count, LANES), 1) + (lag & (LANES - 1))
    within = reach < LANES
    lane = reach & (LANES - 1)
    whole = [
        jnp.where(none, v[j], jnp.where(one, v[j + 1], v[min(j + 2, tiles + 1)]))
        for j in range(tiles + 1)
    ]
    fine = [jnp.take_along_axis(t, lane, axis=1, mode="promise_in_bounds") for t in whole]
    return [jnp.where(within, fine[j], fine[j + 1]) for j in range(tiles)]


def stack_rows(correlation, lags, first, templates_of, target, scale):
    stations = correlation.shape[0]
    width = target.shape[1]
    count = 16

    def block(i, _):
        to = pl.multiple_of(i * count, count)
        template = pl.multiple_of(templates_of(i), count)
        total = shifted(correlation, lags, 0, first + to, template, count, width)
        for s in range(1, stations):
            more = shifted(correlation, lags, s, first + to, template, count, width)
            total = [a + b for a, b in zip(total, more)]
        for j, t in enumerate(total):
            target[pl.ds(to, count), pl.ds(j * LANES, LANES)] = (t * scale).astype(target.dtype)
        return 0

    lax.fori_loop(0, target.shape[0] // count, block, 0, unroll=8)


def place():
    me = lax.axis_index("sta")
    return me & 1, (me >> 1) & 1, me >> 2


def rows_of(owned, block_of):
    per = owned // 16
    return lambda i: block_of(i // per) * owned + i % per * 16


def correlate(owned, unit, lagged, block_of, correlation):
    for s in range(unit.shape[0]):
        blocks = [
            unit[s, pl.ds(pl.multiple_of(block_of(b) * owned, 16), owned), :]
            for b in range(correlation.shape[1] // owned)
        ]
        correlation[s] = jnp.dot(
            jnp.concatenate(blocks, axis=0), lagged[s], preferred_element_type=f32
        )


def quarter_kernel(owned, scale, other_pair, other_core, lagged, unit, lags, target, correlation):
    core, pair, rest = place()
    block_of = lambda b: ((rest ^ b) * 2 + (pair ^ other_pair)) * 2 + (core ^ other_core)
    correlate(owned, unit, lagged, block_of, correlation)
    stack_rows(correlation, lags, 0, rows_of(owned, block_of), target, scale)


def first_kernel(
    owned, scale, masked, kept, following, unit, lags, lagged, away, correlation, staggered, inverse,
):
    lag_matrix(masked, kept, following, staggered, inverse, lagged)
    quarter_kernel(owned, scale, 1, 1, lagged, unit, lags, away, correlation)


def sum_kernel(first, home, core, pair, *targets):
    for k, target in enumerate(targets):
        owned = target.shape[0]
        here, there = pl.ds((first + k) * owned, owned), pl.ds(k * owned, owned)
        total = home[here, :] + core[here, :].astype(f32) + pair[there, :].astype(f32)
        target[...] = total.astype(target.dtype)


def shards(records, templates, moveout, gap_start, gap_length):
    stations, _, width = records.shape
    number = templates.shape[0]
    full = width + MAXMO
    devices = lax.axis_size("tm")
    groups = lax.axis_size("sta")
    owned = number // groups
    rest = groups // 4
    scale = math.sqrt(TEMPLATE_LEN / (3.0 * stations * groups))
    own = records.transpose(1, 0, 2)
    following = lax.ppermute(own, "tm", [(i, (i - 1) % devices) for i in range(devices)])
    vmem = pl.BlockSpec(memory_space=pltpu.VMEM)
    hbm = pl.BlockSpec(memory_space=pltpu.HBM)
    depth = CHANNELS * PADDED

    def call(kernel, outs, ins, scratch=(), flops=10**9):
        return pl.pallas_call(
            kernel,
            out_shape=tuple(jax.ShapeDtypeStruct(shape, dtype) for shape, dtype in outs),
            in_specs=ins,
            out_specs=tuple(vmem for _ in outs),
            scratch_shapes=scratch,
            compiler_params=pltpu.CompilerParams(vmem_limit_bytes=24 * 1024 * 1024),
            cost_estimate=pl.CostEstimate(flops=flops, bytes_accessed=2 * 10**6, transcendentals=0),
        )

    flat = templates.transpose(2, 3, 1, 0).reshape(CHANNELS, TEMPLATE_LEN, stations, number // LANES, LANES)
    flat = flat.transpose(0, 1, 3, 2, 4).reshape(CHANNELS, TEMPLATE_LEN * stations * number // LANES, LANES)
    unit, lags, kept, masked = call(
        setup_kernel,
        [
            ((stations, number, depth), bf16),
            ((stations, number, LANES), i32),
            ((8, width), f32),
            ((8, width), f32),
        ],
        [hbm] * 5,
        [
            pltpu.VMEM((CHANNELS, TEMPLATE_LEN * stations * number // LANES, LANES), bf16),
            pltpu.VMEM((stations, number), i32),
            pltpu.SMEM((stations, CHANNELS), i32),
            pltpu.SMEM((stations, CHANNELS), i32),
            pltpu.VMEM((CHANNELS, stations, width), bf16),
            pltpu.VMEM((TEMPLATE_LEN * stations * number // LANES, LANES), f32),
            pltpu.VMEM((stations, number // LANES, depth, LANES), bf16),
            pltpu.VMEM((8, number), f32),
            pltpu.VMEM((8, width), f32),
            pltpu.SemaphoreType.DMA((CHANNELS + 4,)),
        ],
    )(
        *(
            pltpu.with_memory_space_constraint(a, pltpu.HBM)
            for a in (flat, moveout.T, gap_start, gap_length, own)
        )
    )
    quarter = (number // 4, width)
    columns = pltpu.VMEM((stations, number // 4, full), f32)
    lagged, away = call(
        functools.partial(first_kernel, owned, scale),
        [((stations, depth, full), bf16), (quarter, bf16)],
        [vmem] * 5,
        [columns, pltpu.VMEM((2 * width // LANES, 8 * PITCH, LANES), f32), pltpu.VMEM((8, full), f32)],
    )(masked, kept, following, unit, lags)

    def exchange(value, bit):
        return lax.ppermute(value, "sta", [(i, i ^ bit) for i in range(groups)])

    def stacked(other_pair, other_core, dtype):
        kernel = functools.partial(quarter_kernel, owned, scale, other_pair, other_core)
        return call(kernel, [(quarter, dtype)], [vmem] * 3, [columns])(lagged, unit, lags)[0]

    from_core = exchange(away, 1)
    away = stacked(0, 1, bf16)
    to_pair = stacked(1, 0, f32)
    far = rest - 1
    at = far * owned
    from_far = exchange((to_pair[at:] + from_core[at:].astype(f32)).astype(bf16), 2)
    from_near = exchange((to_pair[:at] + from_core[:at].astype(f32)).astype(bf16), 2)
    home = stacked(0, 0, f32)
    from_core = exchange(away, 1)
    block = (owned, width)
    fars = call(
        functools.partial(sum_kernel, far), [(block, bf16)] * (rest - far), [vmem] * 3
    )(home, from_core, from_far)
    arrived = [exchange(fars[k - far], 4 * k) for k in range(rest - 1, far - 1, -1)]
    mine, *nears = call(
        functools.partial(sum_kernel, 0), [(block, f32)] + [(block, bf16)] * (far - 1), [vmem] * 3
    )(home, from_core, from_near)
    arrived += [exchange(nears[k - 1], 4 * k) for k in range(far - 1, 0, -1)]
    for part in arrived:
        mine = mine + part.astype(f32)
    return mine


def solution(mesh):
    placed = (
        P("sta", None, "tm"),
        P(None, "sta", None, None),
        P(None, "sta"),
        P("sta", None),
        P("sta", None),
    )
    return jax.shard_map(
        shards, mesh=mesh, in_specs=placed, out_specs=P("sta", "tm"), check_vma=False
    )
```
